128 devices in a mesh: rep: 2 (over core), dp: 64 (over x, y, z).
Axes of the slice: x: 4, y: 4, z: 4, core: 2. Of those that a mesh axis runs over, the one named last changes fastest.
Arguments:
- a: bfloat16 [128, 2, 4096, 1024], P(('rep', 'dp')), parts along dimension 0
- g: bfloat16 [128, 2, 4096, 4096], P(('rep', 'dp')), parts along dimension 0
Outputs:
- output: bfloat16 [4, 1024, 4096], P('rep'), parts along dimension 0
There are 2 independent parts. The reference program is written for one: setup_inputs(seed, part) draws one part's arguments, and reference() takes and returns one part's arrays. A program takes and returns all parts, laid end to end along the dimension named above; each array names one.
All inputs are finite; a program needn't handle non-finite values.
Results may differ from the reference program's by a relative error of at most 0.012.
Values are sent between devices in bfloat16 or wider.
A program may use at most 1.5 GiB of HBM per device.

```python
import jax
import jax.numpy as jnp
from jax import lax

DEVICES = 64
MATRICES = 2
TOKENS = 4096
D = 1024
FF = 4096


def setup_inputs(seed: int = 0, part: int = 0) -> dict:
    ka, kg, ks = (jax.random.fold_in(k, part) for k in jax.random.split(jax.random.key(seed), 3))
    size = 2.0 ** jax.random.uniform(ks, (DEVICES, MATRICES, 1, 1), jnp.float32, -1.0, 1.0)
    a = jax.random.normal(ka, (DEVICES, MATRICES, TOKENS, D), jnp.float32)
    g = size * jax.random.normal(kg, (DEVICES, MATRICES, TOKENS, FF), jnp.float32) * (DEVICES * TOKENS) ** -0.5
    return {"a": a.astype(jnp.bfloat16), "g": g.astype(jnp.bfloat16)}


def reference(a, g):
    def take(so_far, one):
        term = jnp.einsum("ntd,ntf->ndf", *one, preferred_element_type=jnp.float32).astype(jnp.bfloat16)
        return so_far + term.astype(jnp.float32), None

    return lax.scan(take, jnp.zeros((MATRICES, D, FF), jnp.float32), (a, g))[0].astype(jnp.bfloat16)
```

```python
import functools

import jax
import jax.numpy as jnp
from jax import lax
from jax.experimental import pallas as pl
from jax.experimental.pallas import tpu as pltpu
from jax.sharding import PartitionSpec as P

F32, BF16 = jnp.float32, jnp.bfloat16

WAVE = 1024
NB = 256
SUBS = WAVE // NB
WIDTHS = (384, 384, 256)
STARTS = (0, 384, 768)
SLOTS = 5
GBUF = 3
KB = 512
A_L, A_R, FIN, B_L, B_R, FIN2, RS3, AG3, F2_L, F2_R, REST2, F1_L, F1_R, REST1 = range(14)


def kernel(
    waves, per, a_hbm, g_hbm, out_hbm,
    at, abuf, gbuf, T, R1, R2, R3, O,
    a_sem, g_sem, o_sem, rs_send, ag_send, recv,
):
    rep, me = lax.axis_index("rep"), lax.axis_index("dp")
    x, y, z = me // 16, (me // 4) % 4, me % 4
    tokens = a_hbm.shape[2]

    def place(k):
        p = jnp.where(k == 0, x, jnp.where(k == 1, y, z))
        s = jnp.where(k == 0, 16, jnp.where(k == 1, 4, 1))
        return p, s

    def peer(k, d):
        p, s = place(k)
        return me + ((p + d) % 4 - p) * s

    barrier = pltpu.get_barrier_semaphore()
    for k in range(3):
        for d in (1, 2, 3):
            pl.semaphore_signal(barrier, inc=1, device_id={"dp": peer(k, d)})

    def a_copy(n, i):
        return pltpu.make_async_copy(
            a_hbm.at[0, n, pl.ds(pl.multiple_of(i * KB, KB), KB), :], abuf.at[i % 2], a_sem.at[i % 2]
        )

    def g_copy(j):
        w, s = j // SUBS, j % SUBS
        n = w // per
        col = pl.multiple_of((w % per) * WAVE + s * NB, NB)
        return pltpu.make_async_copy(g_hbm.at[0, n, :, pl.ds(col, NB)], gbuf.at[j % GBUF], g_sem.at[j % GBUF])

    def o_copy(w):
        n = w // per
        col = pl.multiple_of((w % per) * WAVE, WAVE)
        return pltpu.make_async_copy(O.at[w], out_hbm.at[n, :, pl.ds(col, WAVE)], o_sem.at[w])

    def turn(n):
        pieces = tokens // KB

        def piece(i, _):
            a_copy(n, i).wait()
            at[:, pl.ds(pl.multiple_of(i * KB, KB), KB)] = abuf[i % 2].T

            @pl.when(i + 2 < pieces)
            def _():
                a_copy(n, i + 2).start()

            return 0

        lax.fori_loop(0, pieces, piece, 0)

    def send(src, dst, k, d, ssem, rsem):
        pltpu.make_async_remote_copy(
            src_ref=src, dst_ref=dst, send_sem=ssem, recv_sem=rsem, device_id={"dp": peer(k, d)},
        ).start()

    def wait(ref, sem):
        pltpu.make_async_copy(ref, ref, sem).wait()

    def rows(start, size):
        return pl.ds(pl.multiple_of(start, 16), size)

    def add(dst, drow, srcs, n, cols, out=None):
        out = dst if out is None else out
        step = min(n, 64)

        def body(i, _):
            o = i * step
            total = dst[rows(drow + o, step), cols].astype(F32)
            for ref, row in srcs:
                total = total + ref[rows(row + o, step), cols].astype(F32)
            out[rows(drow + o, step), cols] = total.astype(BF16)
            return 0

        if n == step:
            body(0, 0)
        else:
            lax.fori_loop(0, n // step, body, 0)

    def colours(w):
        for c in range(3):
            k0 = (c + w + rep) % 3
            k1, k2 = (k0 + 1) % 3, (k0 + 2) % 3
            yield c, (k0, k1, k2), pl.ds(STARTS[c], WIDTHS[c])

    def rs_first(w, c, k, base, q, t, r, cols, fin):
        p, _ = place(k)
        h = q // 2
        opp, nxt, prv = ((p + i) % 4 for i in (2, 1, 3))
        s = rs_send.at[w]
        al, ar = fin - 2, fin - 1
        send(t.at[rows(base + opp * q, h), cols], r.at[pl.ds(0, h), cols], k, 1, s, recv.at[w, c, al])
        send(t.at[rows(base + opp * q + h, h), cols], r.at[pl.ds(h, h), cols], k, 3, s, recv.at[w, c, ar])
        send(t.at[rows(base + nxt * q + h, h), cols], r.at[pl.ds(3 * h, h), cols], k, 1, s, recv.at[w, c, fin])
        send(t.at[rows(base + prv * q, h), cols], r.at[pl.ds(4 * h, h), cols], k, 3, s, recv.at[w, c, fin])

    def rs_middle(w, c, k, base, q, t, r, cols, fin):
        p, _ = place(k)
        h = q // 2
        nxt, prv = (p + 1) % 4, (p + 3) % 4
        s = rs_send.at[w]
        wait(r.at[pl.ds(0, h), cols], recv.at[w, c, fin - 2])
        add(t, base + nxt * q, [(r, 0)], h, cols)
        wait(r.at[pl.ds(h, h), cols], recv.at[w, c, fin - 1])
        add(t, base + prv * q + h, [(r, h)], h, cols)
        send(t.at[rows(base + nxt * q, h), cols], r.at[pl.ds(2 * h, h), cols], k, 1, s, recv.at[w, c, fin])
        send(t.at[rows(base + prv * q + h, h), cols], r.at[pl.ds(5 * h, h), cols], k, 3, s, recv.at[w, c, fin])

    def rs_last(w, c, k, base, q, t, r, cols, fin):
        p, _ = place(k)
        wait(r.at[pl.ds(q, 2 * q), cols], recv.at[w, c, fin])
        add(t, base + p * q, [(r, q), (r, 2 * q)], q, cols)

    def ag_first(w, c, k, base, q, o, cols, rest):
        p, _ = place(k)
        h = q // 2
        s = ag_send.at[w]
        lo, hi = o.at[rows(base + p * q, h), cols], o.at[rows(base + p * q + h, h), cols]
        send(lo, lo, k, 1, s, recv.at[w, c, rest - 2])
        send(hi, hi, k, 3, s, recv.at[w, c, rest - 1])
        send(hi, hi, k, 1, s, recv.at[w, c, rest])
        send(lo, lo, k, 3, s, recv.at[w, c, rest])

    def ag_middle(w, c, k, base, q, o, cols, rest):
        p, _ = place(k)
        h = q // 2
        s = ag_send.at[w]
        lo = o.at[rows(base + (p + 3) % 4 * q, h), cols]
        hi = o.at[rows(base + (p + 1) % 4 * q + h, h), cols]
        wait(lo, recv.at[w, c, rest - 2])
        send(lo, lo, k, 1, s, recv.at[w, c, rest])
        wait(hi, recv.at[w, c, rest - 1])
        send(hi, hi, k, 3, s, recv.at[w, c, rest])

    def ag_last(w, c, q, o, cols, rest):
        wait(o.at[pl.ds(0, 2 * q), cols], recv.at[w, c, rest])

    def stage(j, w):
        t, o = T.at[w % SLOTS], O.at[w]
        r1, r2, r3 = R1.at[w], R2.at[w], R3.at[w]
        if j == 10:
            for c, ks, cols in colours(w):
                ag_last(w, c, 256, o, cols, REST1)
            o_copy(w).start()
            return
        for c, (k0, k1, k2), cols in colours(w):
            p0, p1, p2 = place(k0)[0], place(k1)[0], place(k2)[0]
            b1 = p0 * 256
            b2 = b1 + p1 * 64
            own = b2 + p2 * 16
            if j == 0:
                rs_first(w, c, k0, 0, 256, t, r1, cols, FIN)
            elif j == 1:
                rs_middle(w, c, k0, 0, 256, t, r1, cols, FIN)
            elif j == 2:
                rs_last(w, c, k0, 0, 256, t, r1, cols, FIN)
                rs_first(w, c, k1, b1, 64, t, r2, cols, FIN2)
            elif j == 3:
                rs_middle(w, c, k1, b1, 64, t, r2, cols, FIN2)
            elif j == 4:
                rs_last(w, c, k1, b1, 64, t, r2, cols, FIN2)
                for d in (1, 2, 3):
                    send(
                        t.at[rows(b2 + (p2 + d) % 4 * 16, 16), cols], r3.at[pl.ds((d - 1) * 16, 16), cols],
                        k2, d, rs_send.at[w], recv.at[w, c, RS3],
                    )
            elif j == 5:
                wait(r3.at[:, cols], recv.at[w, c, RS3])
                add(t, own, [(r3, 0), (r3, 16), (r3, 32)], 16, cols, o)
                mine = o.at[rows(own, 16), cols]
                for d in (1, 2, 3):
                    send(mine, mine, k2, d, ag_send.at[w], recv.at[w, c, AG3])
            elif j == 6:
                wait(r3.at[:, cols], recv.at[w, c, AG3])
                ag_first(w, c, k1, b1, 64, o, cols, REST2)
            elif j == 7:
                ag_middle(w, c, k1, b1, 64, o, cols, REST2)
            elif j == 8:
                ag_last(w, c, 64, o, cols, REST2)
                ag_first(w, c, k0, 0, 256, o, cols, REST1)
            elif j == 9:
                ag_middle(w, c, k0, 0, 256, o, cols, REST1)

    for i in range(2):
        a_copy(0, i).start()
    for j in range(GBUF - 1):
        g_copy(j).start()
    pl.semaphore_wait(barrier, 9)

    steps = waves * SUBS

    def tick(w, _):
        for s in range(SUBS):
            j = w * SUBS + s

            @pl.when(w < waves)
            def _():
                if s == 0:
                    @pl.when(w % per == 0)
                    def _():
                        turn(w // per)

                    @pl.when(w % per == 1)
                    def _():
                        @pl.when(w // per + 1 < waves // per)
                        def _():
                            for i in range(2):
                                a_copy(w // per + 1, i).start()

                    @pl.when(w >= SLOTS)
                    def _():
                        wait(T.at[w % SLOTS, pl.ds(0, 1008), :], rs_send.at[w - SLOTS])

                @pl.when(j + GBUF - 1 < steps)
                def _():
                    g_copy(j + GBUF - 1).start()

                g_copy(j).wait()
                T[w % SLOTS, :, s * NB:(s + 1) * NB] = jnp.dot(
                    at[...], gbuf[j % GBUF], preferred_element_type=F32
                ).astype(BF16)

            for i in reversed(range(11)):
                if (SUBS - 1 + i) % SUBS == s:
                    v = w - (SUBS - 1 + i) // SUBS

                    @pl.when((v >= 0) & (v < waves))
                    def _():
                        stage(i, v)
        return 0

    lax.fori_loop(0, waves + (SUBS - 1 + 10) // SUBS, tick, 0)

    def finish(w, _):
        @pl.when(w >= waves - SLOTS)
        def _():
            wait(T.at[w % SLOTS, pl.ds(0, 1008), :], rs_send.at[w])

        wait(O.at[w, pl.ds(0, 1008), :], ag_send.at[w])
        o_copy(w).wait()
        return 0

    lax.fori_loop(0, waves, finish, 0)


def solution(mesh):
    def body(a, g):
        _, mats, tokens, d = a.shape
        ff = g.shape[3]
        per = ff // WAVE
        waves = mats * per
        dma = pltpu.SemaphoreType.DMA
        return pl.pallas_call(
            functools.partial(kernel, waves, per),
            name="sums",
            out_shape=jax.ShapeDtypeStruct((mats, d, ff), BF16),
            in_specs=[pl.BlockSpec(memory_space=pl.ANY)] * 2,
            out_specs=pl.BlockSpec(memory_space=pl.ANY),
            scratch_shapes=[
                pltpu.VMEM((d, tokens), BF16),
                pltpu.VMEM((2, KB, d), BF16),
                pltpu.VMEM((GBUF, tokens, NB), BF16),
                pltpu.VMEM((SLOTS, d, WAVE), BF16),
                pltpu.VMEM((waves, 768, WAVE), BF16),
                pltpu.VMEM((waves, 192, WAVE), BF16),
                pltpu.VMEM((waves, 48, WAVE), BF16),
                pltpu.VMEM((waves, d, WAVE), BF16),
                dma((2,)),
                dma((GBUF,)),
                dma((waves,)),
                dma((waves,)),
                dma((waves,)),
                dma((waves, 3, 14)),
            ],
            compiler_params=pltpu.CompilerParams(
                collective_id=0, has_side_effects=True, vmem_limit_bytes=67_043_328
            ),
            cost_estimate=pl.CostEstimate(
                flops=2 * mats * tokens * d * ff, bytes_accessed=2 * mats * tokens * (d + ff), transcendentals=0
            ),
        )(a, g)

    return jax.shard_map(
        body, mesh=mesh, in_specs=P(("rep", "dp"), None, None, None), out_specs=P("rep", None, None), check_vma=False
    )
```

```python
import functools

import jax
import jax.numpy as jnp
from jax import lax
from jax.experimental import pallas as pl
from jax.experimental.pallas import tpu as pltpu
from jax.sharding import PartitionSpec as P

F32, BF16 = jnp.float32, jnp.bfloat16

WAVE = 512
NB = 512
SUBS = WAVE // NB
WIDTHS = (128, 128, 256)
STARTS = (0, 128, 256)
SLOTS = 9
GBUF = 2
ABUF = 4
KB = 512
STAGES = tuple(
    (name, c, first, 1)
    for name, first in (
        ("rs1a", 0), ("ag3", 5), ("rs3", 4), ("rs2c", 3), ("rs2a", 2), ("ag2a", 6), ("ag2c", 7), ("rs1c", 1), ("rs1b", 0),
        ("ag1a", 8), ("ag1b", 8), ("ag1c", 9), ("done", 10),
    )
    for c in range(3)
)
A_L, A_R, FIN, B_L, B_R, FIN2, RS3, AG3, F2_L, F2_R, REST2, F1_L, F1_R, REST1 = range(14)


def kernel(
    waves, per, a_hbm, g_hbm, O,
    at, abuf, gbuf, T, R1, R2, R3,
    a_sem, g_sem, rs_send, ag_send, recv,
):
    rep, me = lax.axis_index("rep"), lax.axis_index("dp")
    tokens = a_hbm.shape[2]

    coords = (lax.div(me, 16), lax.rem(lax.div(me, 4), 4), lax.rem(me, 4))
    spot = tuple(tuple(lax.rem(p + d, 4) for p in coords) for d in range(4))
    peer = tuple(tuple(me + (spot[d][k] - coords[k]) * (16, 4, 1)[k] for k in range(3)) for d in range(4))

    barrier = pltpu.get_barrier_semaphore()
    for k in range(3):
        for d in (1, 2, 3):
            pl.semaphore_signal(barrier, inc=1, device_id={"dp": peer[d][k]})

    def a_copy(n, i):
        return pltpu.make_async_copy(
            a_hbm.at[0, n, pl.ds(pl.multiple_of(i * KB, KB), KB), :], abuf.at[lax.rem(i, ABUF)], a_sem.at[lax.rem(i, ABUF)]
        )

    def g_copy(j):
        w, s = lax.div(j, SUBS), lax.rem(j, SUBS)
        n = lax.div(w, per)
        col = pl.multiple_of((lax.rem(w, per)) * WAVE + s * NB, NB)
        return pltpu.make_async_copy(g_hbm.at[0, n, :, pl.ds(col, NB)], gbuf.at[lax.rem(j, GBUF)], g_sem.at[lax.rem(j, GBUF)])

    def place_out(w):
        return lax.div(w, per), (lax.rem(w, per)) * WAVE

    def turn(n):
        pieces = tokens // KB

        def piece(i, _):
            a_copy(n, i).wait()
            at[:, pl.ds(pl.multiple_of(i * KB, KB), KB)] = abuf[lax.rem(i, ABUF)].T

            @pl.when(i + ABUF < pieces)
            def _():
                a_copy(n, i + ABUF).start()

            return 0

        lax.fori_loop(0, pieces, piece, 0)

    def send(src, dst, to, ssem, rsem):
        pltpu.make_async_remote_copy(
            src_ref=src, dst_ref=dst, send_sem=ssem, recv_sem=rsem, device_id={"dp": to},
        ).start()

    def wait(ref, sem):
        pltpu.make_async_copy(ref, ref, sem).wait()

    def rows(start, size):
        return pl.ds(pl.multiple_of(start, 16), size)

    def add(dst, drow, srcs, n, cols, out=None, out_cols=None):
        out, out_cols = (dst, cols) if out is None else (out, out_cols)
        step = min(n, 128)

        def body(i, _):
            o = i * step
            total = dst[rows(drow + o, step), cols].astype(F32)
            for ref, row in srcs:
                total = total + ref[rows(row + o, step), cols].astype(F32)
            out[rows(drow + o, step), out_cols] = total.astype(BF16)
            return 0

        if n == step:
            body(0, 0)
        else:
            lax.fori_loop(0, n // step, body, 0)

    class Axis:
        def __init__(self, r, c, i):
            self.pick = lambda v: jnp.where(
                r == 0, v[(c + i) % 3], jnp.where(r == 1, v[(c + i + 1) % 3], v[(c + i + 2) % 3])
            )

        def at(self, d):
            return self.pick(spot[d])

        def to(self, d):
            return self.pick(peer[d])

    def rs_first(x, base, q, t, r, cols, s, al, ar):
        h = q // 2
        row = base + x.at(2) * q
        send(t.at[rows(row, h), cols], r.at[pl.ds(0, h), cols], x.to(1), s, al)
        send(t.at[rows(row + h, h), cols], r.at[pl.ds(h, h), cols], x.to(3), s, ar)

    def rs_second(x, base, q, t, r, cols, s, fin):
        h = q // 2
        send(t.at[rows(base + x.at(1) * q + h, h), cols], r.at[pl.ds(3 * h, h), cols], x.to(1), s, fin)
        send(t.at[rows(base + x.at(3) * q, h), cols], r.at[pl.ds(4 * h, h), cols], x.to(3), s, fin)

    def rs_middle(x, base, q, t, r, cols, s, al, ar, fin):
        h = q // 2
        one, two = base + x.at(1) * q, base + x.at(3) * q + h
        wait(r.at[pl.ds(0, h), cols], al)
        add(t, one, [(r, 0)], h, cols)
        wait(r.at[pl.ds(h, h), cols], ar)
        add(t, two, [(r, h)], h, cols)
        send(t.at[rows(one, h), cols], r.at[pl.ds(2 * h, h), cols], x.to(1), s, fin)
        send(t.at[rows(two, h), cols], r.at[pl.ds(5 * h, h), cols], x.to(3), s, fin)

    def rs_last(x, base, q, t, r, cols, fin):
        wait(r.at[pl.ds(q, 2 * q), cols], fin)
        add(t, base + x.at(0) * q, [(r, q), (r, 2 * q)], q, cols)

    def ag_parts(x, base, q, o, cols, d):
        h = q // 2
        row = base + x.at(d) * q
        return o.at[rows(row, h), cols], o.at[rows(row + h, h), cols]

    def ag_first(x, base, q, o, cols, s, fl, fr):
        lo, hi = ag_parts(x, base, q, o, cols, 0)
        send(lo, lo, x.to(1), s, fl)
        send(hi, hi, x.to(3), s, fr)

    def ag_second(x, base, q, o, cols, s, rest):
        lo, hi = ag_parts(x, base, q, o, cols, 0)
        send(hi, hi, x.to(1), s, rest)
        send(lo, lo, x.to(3), s, rest)

    def ag_middle(x, base, q, o, cols, s, fl, fr, rest):
        lo, _ = ag_parts(x, base, q, o, cols, 3)
        _, hi = ag_parts(x, base, q, o, cols, 1)
        wait(lo, fl)
        send(lo, lo, x.to(1), s, rest)
        wait(hi, fr)
        send(hi, hi, x.to(3), s, rest)

    def ag_last(q, o, cols, rest):
        wait(o.at[pl.ds(0, 2 * q), cols], rest)

    def stage(name, c, w):
        n, col = place_out(w)
        t, o = T.at[lax.rem(w, SLOTS)], O.at[n]
        r1, r2, r3 = R1.at[w], R2.at[w], R3.at[w]
        turn_of = lax.rem(w + rep, 3)
        rs, ag = rs_send.at[w], ag_send.at[w]
        rv = recv.at[w, c]
        cols = pl.ds(STARTS[c], WIDTHS[c])
        ocols = pl.ds(pl.multiple_of(col + STARTS[c], 128), WIDTHS[c])
        x0, x1, x2 = (Axis(turn_of, c, i) for i in range(3))
        if name == "rs1a":
            rs_first(x0, 0, 256, t, r1, cols, rs, rv.at[A_L], rv.at[A_R])
        elif name == "rs1b":
            rs_second(x0, 0, 256, t, r1, cols, rs, rv.at[FIN])
        elif name == "rs1c":
            rs_middle(x0, 0, 256, t, r1, cols, rs, rv.at[A_L], rv.at[A_R], rv.at[FIN])
        elif name == "ag1b":
            ag_second(x0, 0, 256, o, ocols, ag, rv.at[REST1])
        elif name == "ag1c":
            ag_middle(x0, 0, 256, o, ocols, ag, rv.at[F1_L], rv.at[F1_R], rv.at[REST1])
        elif name == "ag1a":
            ag_last(64, o, ocols, rv.at[REST2])
            ag_first(x0, 0, 256, o, ocols, ag, rv.at[F1_L], rv.at[F1_R])
        elif name == "done":
            ag_last(256, o, ocols, rv.at[REST1])
        else:
            b1 = x0.at(0) * 256
            if name == "rs2a":
                rs_last(x0, 0, 256, t, r1, cols, rv.at[FIN])
                rs_first(x1, b1, 64, t, r2, cols, rs, rv.at[B_L], rv.at[B_R])
                rs_second(x1, b1, 64, t, r2, cols, rs, rv.at[FIN2])
            elif name == "rs2c":
                rs_middle(x1, b1, 64, t, r2, cols, rs, rv.at[B_L], rv.at[B_R], rv.at[FIN2])
            elif name == "ag2a":
                wait(r3.at[:, cols], rv.at[AG3])
                ag_first(x1, b1, 64, o, ocols, ag, rv.at[F2_L], rv.at[F2_R])
                ag_second(x1, b1, 64, o, ocols, ag, rv.at[REST2])
            elif name == "ag2c":
                ag_middle(x1, b1, 64, o, ocols, ag, rv.at[F2_L], rv.at[F2_R], rv.at[REST2])
            elif name == "rs3":
                rs_last(x1, b1, 64, t, r2, cols, rv.at[FIN2])
                b2 = b1 + x1.at(0) * 64
                for d in (1, 2, 3):
                    piece = t.at[rows(b2 + x2.at(d) * 16, 16), cols]
                    send(piece, r3.at[pl.ds((d - 1) * 16, 16), cols], x2.to(d), rs, rv.at[RS3])
            elif name == "ag3":
                own = b1 + x1.at(0) * 64 + x2.at(0) * 16
                wait(r3.at[:, cols], rv.at[RS3])
                add(t, own, [(r3, 0), (r3, 16), (r3, 32)], 16, cols, o, ocols)
                mine = o.at[rows(own, 16), ocols]
                for d in (1, 2, 3):
                    send(mine, mine, x2.to(d), ag, rv.at[AG3])

    for i in range(ABUF):
        a_copy(0, i).start()
    for j in range(GBUF - 1):
        g_copy(j).start()
    pl.semaphore_wait(barrier, 9)

    steps = waves * SUBS

    def tick(j, _):
        @pl.when(j < steps)
        def _():
            w, s = lax.div(j, SUBS), lax.rem(j, SUBS)

            @pl.when(s == 0)
            def _():
                @pl.when(lax.rem(w, per) == 0)
                def _():
                    turn(lax.div(w, per))

                @pl.when((lax.rem(w, per) == 1) & (lax.div(w, per) + 1 < waves // per))
                def _():
                    for i in range(ABUF):
                        a_copy(lax.div(w, per) + 1, i).start()

                @pl.when(w >= SLOTS)
                def _():
                    wait(T.at[lax.rem(w, SLOTS), pl.ds(0, 1008), :], rs_send.at[w - SLOTS])

            @pl.when(j + GBUF - 1 < steps)
            def _():
                g_copy(j + GBUF - 1).start()

            g_copy(j).wait()
            T[lax.rem(w, SLOTS), :, pl.ds(pl.multiple_of(s * NB, NB), NB)] = jnp.dot(
                at[...], gbuf[lax.rem(j, GBUF)], preferred_element_type=F32
            ).astype(BF16)

        for name, c, first, every in STAGES:
            v, odd = lax.div(j - first, every), lax.rem(j - first, every)

            @pl.when((j >= first) & (odd == 0) & (v < waves))
            def _():
                stage(name, c, v)

        return 0

    lax.fori_loop(0, 1 + max(first + every * (waves - 1) for _, _, first, every in STAGES), tick, 0)

    def finish(w, _):
        @pl.when(w >= waves - SLOTS)
        def _():
            wait(T.at[lax.rem(w, SLOTS), pl.ds(0, 1008), :], rs_send.at[w])

        n, col = place_out(w)
        wait(O.at[n, pl.ds(0, 1008), pl.ds(pl.multiple_of(col, WAVE), WAVE)], ag_send.at[w])
        return 0

    lax.fori_loop(0, waves, finish, 0)


def solution(mesh):
    def body(a, g):
        _, mats, tokens, d = a.shape
        ff = g.shape[3]
        per = ff // WAVE
        waves = mats * per
        dma = pltpu.SemaphoreType.DMA
        return pl.pallas_call(
            functools.partial(kernel, waves, per),
            name="sums",
            out_shape=pltpu.VMEM((mats, d, ff), BF16),
            in_specs=[pl.BlockSpec(memory_space=pl.ANY)] * 2,
            out_specs=pl.BlockSpec(memory_space=pltpu.VMEM),
            scratch_shapes=[
                pltpu.VMEM((d, tokens), BF16),
                pltpu.VMEM((ABUF, KB, d), BF16),
                pltpu.VMEM((GBUF, tokens, NB), BF16),
                pltpu.VMEM((SLOTS, d, WAVE), BF16),
                pltpu.VMEM((waves, 768, WAVE), BF16),
                pltpu.VMEM((waves, 192, WAVE), BF16),
                pltpu.VMEM((waves, 48, WAVE), BF16),
                dma((ABUF,)),
                dma((GBUF,)),
                dma((waves,)),
                dma((waves,)),
                dma((waves, 3, 14)),
            ],
            compiler_params=pltpu.CompilerParams(
                collective_id=0, has_side_effects=True, vmem_limit_bytes=49_500_000
            ),
            cost_estimate=pl.CostEstimate(
                flops=2 * mats * tokens * d * ff, bytes_accessed=2 * mats * tokens * (d + ff), transcendentals=0
            ),
        )(a, g)

    return jax.shard_map(
        body, mesh=mesh, in_specs=P(("rep", "dp"), None, None, None), out_specs=P("rep", None, None), check_vma=False
    )
```

```python
import functools

import jax
import jax.numpy as jnp
from jax import lax
from jax.experimental import pallas as pl
from jax.experimental.pallas import tpu as pltpu
from jax.sharding import PartitionSpec as P

F32, BF16 = jnp.float32, jnp.bfloat16

WAVE = 512
NB = 512
SUBS = WAVE // NB
WIDTHS = (128, 128, 256)
STARTS = (0, 128, 256)
SLOTS = 9
GBUF = 2
ABUF = 4
KB = 512
STAGES = tuple(
    (name, c, first, 1)
    for name, first in (
        ("rs1a", 0), ("rs1c", 1), ("ag3", 5), ("rs3", 4), ("rs2c", 3), ("rs2a", 2), ("ag2a", 6), ("ag2c", 7), ("rs1b", 0),
        ("ag1a", 8), ("ag1b", 8), ("ag1c", 10), ("done", 12),
    )
    for c in range(3)
)
A_L, A_R, FIN, B_L, B_R, FIN2, RS3, AG3, F2_L, F2_R, REST2, F1_L, F1_R, REST1 = range(14)


def kernel(
    waves, per, a_hbm, g_hbm, O,
    at, abuf, gbuf, T, R1, R2, R3,
    a_sem, g_sem, rs_send, ag_send, recv,
):
    rep, me = lax.axis_index("rep"), lax.axis_index("dp")
    tokens = a_hbm.shape[2]

    coords = (lax.div(me, 16), lax.rem(lax.div(me, 4), 4), lax.rem(me, 4))
    spot = tuple(tuple(lax.rem(p + d, 4) for p in coords) for d in range(4))
    peer = tuple(tuple(me + (spot[d][k] - coords[k]) * (16, 4, 1)[k] for k in range(3)) for d in range(4))

    barrier = pltpu.get_barrier_semaphore()
    for k in range(3):
        for d in (1, 2, 3):
            pl.semaphore_signal(barrier, inc=1, device_id={"dp": peer[d][k]})

    def a_copy(n, i):
        return pltpu.make_async_copy(
            a_hbm.at[0, n, pl.ds(pl.multiple_of(i * KB, KB), KB), :], abuf.at[lax.rem(i, ABUF)], a_sem.at[lax.rem(i, ABUF)]
        )

    def g_copy(j):
        w, s = lax.div(j, SUBS), lax.rem(j, SUBS)
        n = lax.div(w, per)
        col = pl.multiple_of((lax.rem(w, per)) * WAVE + s * NB, NB)
        return pltpu.make_async_copy(g_hbm.at[0, n, :, pl.ds(col, NB)], gbuf.at[lax.rem(j, GBUF)], g_sem.at[lax.rem(j, GBUF)])

    def place_out(w):
        return lax.div(w, per), (lax.rem(w, per)) * WAVE

    def turn(n):
        pieces = tokens // KB

        def piece(i, _):
            a_copy(n, i).wait()
            at[:, pl.ds(pl.multiple_of(i * KB, KB), KB)] = abuf[lax.rem(i, ABUF)].T

            @pl.when(i + ABUF < pieces)
            def _():
                a_copy(n, i + ABUF).start()

            return 0

        lax.fori_loop(0, pieces, piece, 0)

    def send(src, dst, to, ssem, rsem):
        pltpu.make_async_remote_copy(
            src_ref=src, dst_ref=dst, send_sem=ssem, recv_sem=rsem, device_id={"dp": to},
        ).start()

    def wait(ref, sem):
        pltpu.make_async_copy(ref, ref, sem).wait()

    def rows(start, size):
        return pl.ds(pl.multiple_of(start, 16), size)

    def add(dst, drow, srcs, n, cols, out=None, out_cols=None):
        out, out_cols = (dst, cols) if out is None else (out, out_cols)
        step = min(n, 128)

        def body(i, _):
            o = i * step
            total = dst[rows(drow + o, step), cols].astype(F32)
            for ref, row in srcs:
                total = total + ref[rows(row + o, step), cols].astype(F32)
            out[rows(drow + o, step), out_cols] = total.astype(BF16)
            return 0

        if n == step:
            body(0, 0)
        else:
            lax.fori_loop(0, n // step, body, 0)

    class Axis:
        def __init__(self, r, c, i):
            self.pick = lambda v: jnp.where(
                r == 0, v[(c + i) % 3], jnp.where(r == 1, v[(c + i + 1) % 3], v[(c + i + 2) % 3])
            )

        def at(self, d):
            return self.pick(spot[d])

        def to(self, d):
            return self.pick(peer[d])

    def rs_first(x, base, q, t, r, cols, s, al, ar):
        h = q // 2
        row = base + x.at(2) * q
        send(t.at[rows(row, h), cols], r.at[pl.ds(0, h), cols], x.to(1), s, al)
        send(t.at[rows(row + h, h), cols], r.at[pl.ds(h, h), cols], x.to(3), s, ar)

    def rs_second(x, base, q, t, r, cols, s, fin):
        h = q // 2
        send(t.at[rows(base + x.at(1) * q + h, h), cols], r.at[pl.ds(3 * h, h), cols], x.to(1), s, fin)
        send(t.at[rows(base + x.at(3) * q, h), cols], r.at[pl.ds(4 * h, h), cols], x.to(3), s, fin)

    def rs_middle(x, base, q, t, r, cols, s, al, ar, fin):
        h = q // 2
        one, two = base + x.at(1) * q, base + x.at(3) * q + h
        wait(r.at[pl.ds(0, h), cols], al)
        add(t, one, [(r, 0)], h, cols)
        wait(r.at[pl.ds(h, h), cols], ar)
        add(t, two, [(r, h)], h, cols)
        send(t.at[rows(one, h), cols], r.at[pl.ds(2 * h, h), cols], x.to(1), s, fin)
        send(t.at[rows(two, h), cols], r.at[pl.ds(5 * h, h), cols], x.to(3), s, fin)

    def rs_last(x, base, q, t, r, cols, fin):
        wait(r.at[pl.ds(q, 2 * q), cols], fin)
        add(t, base + x.at(0) * q, [(r, q), (r, 2 * q)], q, cols)

    def ag_parts(x, base, q, o, cols, d):
        h = q // 2
        row = base + x.at(d) * q
        return o.at[rows(row, h), cols], o.at[rows(row + h, h), cols]

    def ag_first(x, base, q, o, cols, s, fl, fr):
        lo, hi = ag_parts(x, base, q, o, cols, 0)
        send(lo, lo, x.to(1), s, fl)
        send(hi, hi, x.to(3), s, fr)

    def ag_second(x, base, q, o, cols, s, rest):
        lo, hi = ag_parts(x, base, q, o, cols, 0)
        send(hi, hi, x.to(1), s, rest)
        send(lo, lo, x.to(3), s, rest)

    def ag_middle(x, base, q, o, cols, s, fl, fr, rest):
        lo, _ = ag_parts(x, base, q, o, cols, 3)
        _, hi = ag_parts(x, base, q, o, cols, 1)
        wait(lo, fl)
        send(lo, lo, x.to(1), s, rest)
        wait(hi, fr)
        send(hi, hi, x.to(3), s, rest)

    def ag_last(q, o, cols, rest):
        wait(o.at[pl.ds(0, 2 * q), cols], rest)

    def stage(name, c, w):
        n, col = place_out(w)
        t, o = T.at[lax.rem(w, SLOTS)], O.at[n]
        r1, r2, r3 = R1.at[w], R2.at[w], R3.at[w]
        turn_of = lax.rem(w + rep, 3)
        rs, ag = rs_send.at[w], ag_send.at[w]
        rv = recv.at[w, c]
        cols = pl.ds(STARTS[c], WIDTHS[c])
        ocols = pl.ds(pl.multiple_of(col + STARTS[c], 128), WIDTHS[c])
        x0, x1, x2 = (Axis(turn_of, c, i) for i in range(3))
        if name == "rs1a":
            rs_first(x0, 0, 256, t, r1, cols, rs, rv.at[A_L], rv.at[A_R])
        elif name == "rs1b":
            rs_second(x0, 0, 256, t, r1, cols, rs, rv.at[FIN])
        elif name == "rs1c":
            rs_middle(x0, 0, 256, t, r1, cols, rs, rv.at[A_L], rv.at[A_R], rv.at[FIN])
        elif name == "ag1b":
            ag_second(x0, 0, 256, o, ocols, ag, rv.at[REST1])
        elif name == "ag1c":
            ag_middle(x0, 0, 256, o, ocols, ag, rv.at[F1_L], rv.at[F1_R], rv.at[REST1])
        elif name == "ag1a":
            ag_last(64, o, ocols, rv.at[REST2])
            ag_first(x0, 0, 256, o, ocols, ag, rv.at[F1_L], rv.at[F1_R])
        elif name == "done":
            ag_last(256, o, ocols, rv.at[REST1])
        else:
            b1 = x0.at(0) * 256
            if name == "rs2a":
                rs_last(x0, 0, 256, t, r1, cols, rv.at[FIN])
                rs_first(x1, b1, 64, t, r2, cols, rs, rv.at[B_L], rv.at[B_R])
                rs_second(x1, b1, 64, t, r2, cols, rs, rv.at[FIN2])
            elif name == "rs2c":
                rs_middle(x1, b1, 64, t, r2, cols, rs, rv.at[B_L], rv.at[B_R], rv.at[FIN2])
            elif name == "ag2a":
                wait(r3.at[:, cols], rv.at[AG3])
                ag_first(x1, b1, 64, o, ocols, ag, rv.at[F2_L], rv.at[F2_R])
                ag_second(x1, b1, 64, o, ocols, ag, rv.at[REST2])
            elif name == "ag2c":
                ag_middle(x1, b1, 64, o, ocols, ag, rv.at[F2_L], rv.at[F2_R], rv.at[REST2])
            elif name == "rs3":
                rs_last(x1, b1, 64, t, r2, cols, rv.at[FIN2])
                b2 = b1 + x1.at(0) * 64
                for d in (1, 2, 3):
                    piece = t.at[rows(b2 + x2.at(d) * 16, 16), cols]
                    send(piece, r3.at[pl.ds((d - 1) * 16, 16), cols], x2.to(d), rs, rv.at[RS3])
            elif name == "ag3":
                own = b1 + x1.at(0) * 64 + x2.at(0) * 16
                wait(r3.at[:, cols], rv.at[RS3])
                add(t, own, [(r3, 0), (r3, 16), (r3, 32)], 16, cols, o, ocols)
                mine = o.at[rows(own, 16), ocols]
                for d in (1, 2, 3):
                    send(mine, mine, x2.to(d), ag, rv.at[AG3])

    for i in range(ABUF):
        a_copy(0, i).start()
    for j in range(GBUF - 1):
        g_copy(j).start()
    pl.semaphore_wait(barrier, 9)

    steps = waves * SUBS

    def tick(j, _):
        @pl.when(j < steps)
        def _():
            w, s = lax.div(j, SUBS), lax.rem(j, SUBS)

            @pl.when(s == 0)
            def _():
                @pl.when(lax.rem(w, per) == 0)
                def _():
                    turn(lax.div(w, per))

                @pl.when((lax.rem(w, per) == 1) & (lax.div(w, per) + 1 < waves // per))
                def _():
                    for i in range(ABUF):
                        a_copy(lax.div(w, per) + 1, i).start()

                @pl.when(w >= SLOTS)
                def _():
                    wait(T.at[lax.rem(w, SLOTS), pl.ds(0, 1008), :], rs_send.at[w - SLOTS])

            @pl.when(j + GBUF - 1 < steps)
            def _():
                g_copy(j + GBUF - 1).start()

            g_copy(j).wait()
            T[lax.rem(w, SLOTS), :, pl.ds(pl.multiple_of(s * NB, NB), NB)] = jnp.dot(
                at[...], gbuf[lax.rem(j, GBUF)], preferred_element_type=F32
            ).astype(BF16)

        for name, c, first, every in STAGES:
            v, odd = lax.div(j - first, every), lax.rem(j - first, every)

            @pl.when((j >= first) & (odd == 0) & (v < waves))
            def _():
                stage(name, c, v)

        return 0

    lax.fori_loop(0, 1 + max(first + every * (waves - 1) for _, _, first, every in STAGES), tick, 0)

    def finish(w, _):
        @pl.when(w >= waves - SLOTS)
        def _():
            wait(T.at[lax.rem(w, SLOTS), pl.ds(0, 1008), :], rs_send.at[w])

        n, col = place_out(w)
        wait(O.at[n, pl.ds(0, 1008), pl.ds(pl.multiple_of(col, WAVE), WAVE)], ag_send.at[w])
        return 0

    lax.fori_loop(0, waves, finish, 0)


def solution(mesh):
    def body(a, g):
        _, mats, tokens, d = a.shape
        ff = g.shape[3]
        per = ff // WAVE
        waves = mats * per
        dma = pltpu.SemaphoreType.DMA
        return pl.pallas_call(
            functools.partial(kernel, waves, per),
            name="sums",
            out_shape=pltpu.VMEM((mats, d, ff), BF16),
            in_specs=[pl.BlockSpec(memory_space=pl.ANY)] * 2,
            out_specs=pl.BlockSpec(memory_space=pltpu.VMEM),
            scratch_shapes=[
                pltpu.VMEM((d, tokens), BF16),
                pltpu.VMEM((ABUF, KB, d), BF16),
                pltpu.VMEM((GBUF, tokens, NB), BF16),
                pltpu.VMEM((SLOTS, d, WAVE), BF16),
                pltpu.VMEM((waves, 768, WAVE), BF16),
                pltpu.VMEM((waves, 192, WAVE), BF16),
                pltpu.VMEM((waves, 48, WAVE), BF16),
                dma((ABUF,)),
                dma((GBUF,)),
                dma((waves,)),
                dma((waves,)),
                dma((waves, 3, 14)),
            ],
            compiler_params=pltpu.CompilerParams(
                collective_id=0, has_side_effects=True, vmem_limit_bytes=49_500_000
            ),
            cost_estimate=pl.CostEstimate(
                flops=2 * mats * tokens * d * ff, bytes_accessed=2 * mats * tokens * (d + ff), transcendentals=0
            ),
        )(a, g)

    return jax.shard_map(
        body, mesh=mesh, in_specs=P(("rep", "dp"), None, None, None), out_specs=P("rep", None, None), check_vma=False
    )
```
